1024 devices in a mesh: outer: 16 (over x, y), inner: 8 (over z_lo), tensor: 8 (over z_hi, core).
Axes of the slice: x: 4, y: 4, z: 32 (z_hi: 4, z_lo: 8; z = z_hi * 8 + z_lo), core: 2. Of those that a mesh axis runs over, the one named last changes fastest.
Arguments:
- queries: bfloat16 [16384, 4096], P(('outer', 'inner'), 'tensor')
- keys: bfloat16 [16384, 1024], P(('outer', 'inner'), 'tensor')
- values: bfloat16 [16384, 1024], P(('outer', 'inner'), 'tensor'), may hold values from -6 to 6
- stretch_order: int32 [256], replicated, may hold values from 0 to 255, as said below
- w_out: bfloat16 [4096, 8192], P('tensor'), may hold values from -0.125 to 0.125
Outputs:
- mixed: bfloat16 [16384, 8192], P(('outer', 'inner'), 'tensor')
The draws below stay inside these ranges and needn't reach their ends.
Inputs may be any that keep to these rules, and one draw needn't show every extreme that they name: stretch_order is a permutation of 0 to 255, and storage stretches 2 d and 2 d + 1 hold sequence stretches j and 255 - j for some j < 128.
All inputs are finite; a program needn't handle non-finite values.
Results may differ from the reference program's by a relative error of at most 0.015.
Values may be sent and summed in bfloat16 or wider, within the bound.
No kernel may reach another device: no remote copies, remote signals or barrier semaphores. Data moves between devices by JAX's collectives and lax.ppermute only.
A program may use at most 64 MiB of HBM per device.

```python
import math
import jax
import jax.numpy as jnp
from jax import lax

D = 8192
QH = 32
KVH = 8
HD = 128
TOK_DEV = 128
CH = 64
TOKENS = 16384
STRETCHES = 256


def paired_draw(key):
    key_q, key_k = jax.random.split(key, 2)
    query_part = jnp.clip(jax.random.normal(key_q, (TOKENS, QH * HD), jnp.float32), -8.0, 8.0)
    key_part = jnp.clip(jax.random.normal(key_k, (TOKENS, KVH * HD), jnp.float32), -8.0, 8.0)
    return (query_part, key_part)


def draw_queries(key, part):
    return paired_draw(jax.random.fold_in(key, 7))[0].astype(jnp.bfloat16)


def draw_keys(key, part):
    return paired_draw(jax.random.fold_in(key, 7))[1].astype(jnp.bfloat16)


def draw_stretch_order(key, part):
    holders = STRETCHES // 2
    order = jax.random.permutation(jax.random.fold_in(key, 11), holders).astype(jnp.int32)
    return jnp.stack([order, STRETCHES - 1 - order], axis=1).reshape(STRETCHES)


def strengthened(entries, stream_key, source, target, shards_of, factor):
    owner, partner = [(jnp.arange(entries.shape[axis_at]) // (entries.shape[axis_at] // shards_of)).reshape([-1 if axis == axis_at else 1 for axis in range(entries.ndim)]) for axis_at in (source, target)]
    chosen = jax.random.permutation(stream_key, shards_of)[partner]
    strong = (owner == chosen) | (owner == (partner + shards_of // 2) % shards_of)
    return jnp.where(strong, factor * entries, entries)


def block_scale(rng, dims, pieces, least, largest):
    gain, own = 1.0, jax.random.fold_in(rng, 6)
    for dim, parts in pieces:
        draws = jnp.exp(jax.random.uniform(jax.random.fold_in(own, dim), (parts,), jnp.float32, least / len(pieces), largest / len(pieces)))
        gain = gain * jnp.repeat(draws, dims[dim] // parts).reshape([-1 if axis == dim else 1 for axis in range(len(dims))])
    return gain


def gaussian(rng, shape, deviation, most, cuts=(), held_as=jnp.bfloat16):
    values = jax.random.normal(rng, shape, jnp.float32) * deviation
    if len(cuts) > 0:
        values = block_scale(rng, shape, cuts, -0.22, 0.18) * values
    return jnp.clip(values, min=-most, max=most).astype(held_as)


def gaussian_with(own_key, shape, deviation, limit, pieces, heavy, kind=jnp.bfloat16):
    drawn = deviation * jax.random.normal(own_key, shape, jnp.float32)
    if pieces:
        drawn = drawn * block_scale(own_key, shape, pieces, -0.22, 0.18)
    return jnp.clip(strengthened(drawn, jax.random.fold_in(own_key, 3), *heavy), -limit, limit).astype(kind)


def setup_inputs(seed: int = 0) -> dict:
    arg_keys = jax.random.split(jax.random.key(seed), 6)
    queries = draw_queries(jax.random.fold_in(arg_keys[5], 71), 0)
    keys = draw_keys(jax.random.fold_in(arg_keys[5], 71), 0)
    values = gaussian(arg_keys[2], (TOKENS, KVH * HD), 1.0, 6.0, ((0, 128), (1, 8)))
    stretch_order = draw_stretch_order(jax.random.fold_in(arg_keys[5], 71), 0)
    w_out = gaussian_with(arg_keys[4], (QH * HD, D), (QH * HD) ** -0.5, 0.125, ((0, 8),), (0, 1, 8, 2.0))
    return dict(queries=queries, keys=keys, values=values, stretch_order=stretch_order, w_out=w_out)


def reference(queries, keys, values, stretch_order, w_out):
    group = QH // KVH
    offsets = jnp.arange(TOKENS, dtype=jnp.int32)
    pos = stretch_order[offsets // CH] * CH + offsets % CH
    scale = 1.0 / math.sqrt(HD)
    key_all = keys.reshape(TOKENS, KVH, HD).astype(jnp.float32)
    val_all = values.reshape(TOKENS, KVH, HD).astype(jnp.float32)
    blocks = TOKENS // TOK_DEV
    q_blocks = queries.reshape(blocks, TOK_DEV, KVH, group, HD)
    p_blocks = pos.reshape(blocks, TOK_DEV)

    def one_block(items):
        q_rows, q_pos = items
        scores = jnp.einsum('rhgd,khd->hrgk', q_rows.astype(jnp.float32), key_all) * scale
        allowed = pos[None, None, None, :] <= q_pos[None, :, None, None]
        scores = jnp.where(allowed, scores, -1e+30)
        top = lax.optimization_barrier(jnp.max(scores, axis=-1, keepdims=True))
        weights = jnp.exp(scores - top) * allowed.astype(jnp.float32)
        total = lax.optimization_barrier(jnp.sum(weights, axis=-1))
        low = weights.astype(jnp.bfloat16).astype(jnp.float32)
        summed = jnp.einsum('hrgk,khd->rhgd', low, val_all)
        result = summed / jnp.transpose(total, (1, 0, 2))[..., None]
        return result.astype(jnp.bfloat16)
    attn = lax.map(one_block, (q_blocks, p_blocks)).reshape(TOKENS, QH * HD)
    return jnp.dot(attn, w_out, preferred_element_type=jnp.float32).astype(jnp.bfloat16)
```

```python
import math

import jax
import jax.numpy as jnp
from jax import lax
from jax.experimental import pallas as pl
from jax.experimental.pallas import tpu as pltpu
from jax.sharding import PartitionSpec as P


HD = 128
HEADS = 4
CH = 64
ROWS = 2 * CH
OUTER = 16
INNER = 8
ZHI = 4
QC = HEADS * CH
EXTRA = 16
NEG = -1e30
COEF = math.log2(math.e) / math.sqrt(HD)
PER = 2
HALF = 512


def dot(a, b, dims):
    return lax.dot_general(a, b, (dims, ((), ())), preferred_element_type=jnp.float32)


def three_terms(x):
    hi = x.astype(jnp.bfloat16)
    rest = x - hi.astype(jnp.float32)
    mid = rest.astype(jnp.bfloat16)
    low = (rest - mid.astype(jnp.float32)).astype(jnp.bfloat16)
    return hi.astype(jnp.float32), mid.astype(jnp.float32), low.astype(jnp.float32)


def attention_kernel(own_ref, sel_ref, q_ref, *refs):
    kv_refs = refs[:INNER]
    late_ref, out_ref, pick, dense, vt_dense, vt_e, vt_l = refs[INNER:]
    step = pl.program_id(0)
    keys_dense = INNER * CH

    @pl.when(step == 0)
    def _():
        zero = jnp.zeros((CH, HD), jnp.bfloat16)
        for s in range(INNER):
            k_e = kv_refs[s][:CH, :]
            k_l = kv_refs[s][CH:ROWS, :]
            pick[s, 0] = jnp.concatenate([k_e, zero], axis=1)
            pick[s, 1] = jnp.concatenate([zero, k_l], axis=1)
            dense[s * CH : (s + 1) * CH, :] = jnp.concatenate([zero, k_e], axis=1)
        dense[keys_dense:, :] = jnp.concatenate([zero, kv_refs[0][CH:ROWS, :]], axis=1)
        v_e = jnp.concatenate([kv_refs[s][ROWS : ROWS + CH, :] for s in range(INNER)], axis=0)
        v_l = jnp.concatenate([kv_refs[s][ROWS + CH :, :] for s in range(INNER)], axis=0)
        t_e = v_e.astype(jnp.float32).T.astype(jnp.bfloat16)
        t_l = v_l.astype(jnp.float32).T.astype(jnp.bfloat16)
        vt_e[...] = t_e
        vt_l[...] = t_l
        vt_dense[:, :keys_dense] = t_e
        vt_dense[:, keys_dense:] = t_l[:, :CH]

    key_at = lax.broadcasted_iota(jnp.int32, (CH, QC), 0)
    query_at = lax.broadcasted_iota(jnp.int32, (CH, QC), 1) % CH
    causal = key_at <= query_at

    for p in range(PER):
        a = step * PER + p
        own = a == own_ref[0]
        q = q_ref[p]
        stacked = [
            jnp.concatenate([q[r : r + CH, h * HD : (h + 1) * HD] for h in range(HEADS)], axis=0)
            for r in (0, CH)
        ]
        q_cat = jnp.concatenate(stacked, axis=1)
        s_dense = dot(dense[...], q_cat, ((1,), (1,)))
        late = [sel_ref[a * INNER + s] > 0 for s in range(INNER)]
        chosen = jnp.concatenate([pick[s, sel_ref[a * INNER + s]] for s in range(INNER)], axis=0)
        s_sel = dot(chosen, q_cat, ((1,), (1,)))
        keep = jnp.where(own, 1, 0)
        s_first = jnp.where(jnp.logical_or(causal, keep == 0), s_sel[:CH], NEG)
        s_extra = jnp.where(jnp.logical_and(causal, keep == 1), s_dense[keys_dense:], NEG)
        blocks = [s_first] + [s_sel[s * CH : (s + 1) * CH] for s in range(1, INNER)]
        tops = [jnp.max(b, axis=0, keepdims=True) for b in blocks]
        m_e = jnp.full((1, QC), NEG, jnp.float32)
        m_l = jnp.maximum(
            jnp.max(s_dense[:keys_dense], axis=0, keepdims=True),
            jnp.max(s_extra, axis=0, keepdims=True),
        )
        for s in range(INNER):
            m_e = jnp.maximum(m_e, jnp.where(late[s], NEG, tops[s]))
            m_l = jnp.maximum(m_l, jnp.where(late[s], tops[s], NEG))
        p_dense = jnp.exp2((s_dense[:keys_dense] - m_l) * COEF)
        p_extra = jnp.exp2((s_extra - m_l) * COEF)
        l_l = jnp.sum(p_dense, axis=0, keepdims=True) + jnp.sum(p_extra, axis=0, keepdims=True)
        l_e = jnp.zeros((1, QC), jnp.float32)
        weights = []
        for s in range(INNER):
            w = jnp.exp2((blocks[s] - jnp.where(late[s], m_l, m_e)) * COEF)
            part = jnp.sum(w, axis=0, keepdims=True)
            l_e = l_e + jnp.where(late[s], 0.0, part)
            l_l = l_l + jnp.where(late[s], part, 0.0)
            weights.append(w.astype(jnp.bfloat16))
        w_sel = jnp.concatenate(weights, axis=0)
        w_dense = jnp.concatenate([p_dense.astype(jnp.bfloat16), p_extra.astype(jnp.bfloat16)], axis=0)
        is_late = late_ref[p, 0:1, :]
        v_sel = jnp.concatenate([vt_e[...] * (1 - is_late), vt_l[...] * is_late], axis=0)
        o_sel = dot(v_sel, w_sel, ((1,), (0,)))
        o_e = o_sel[:HD]
        o_l = o_sel[HD:] + dot(vt_dense[...], w_dense, ((1,), (0,)))
        some = l_e > 0.0
        inv_e = jnp.where(some, 1.0 / jnp.where(some, l_e, 1.0), 0.0)
        lse_e = jnp.where(some, m_e * COEF + jnp.log2(jnp.where(some, l_e, 1.0)), NEG)
        lse_l = m_l * COEF + jnp.log2(l_l)
        out_ref[p, :HD, :] = (o_e * inv_e).astype(jnp.bfloat16)
        out_ref[p, HD : 2 * HD, :] = (o_l * (1.0 / l_l)).astype(jnp.bfloat16)
        rows = list(three_terms(lse_e)) + list(three_terms(lse_l))
        rows.append(jnp.zeros((EXTRA - 6, QC), jnp.float32))
        out_ref[p, 2 * HD :, :] = jnp.concatenate(rows, axis=0).astype(jnp.bfloat16)


def partial_attention(own, sel, q_all, kv, late):
    n_keys = INNER * CH
    return pl.pallas_call(
        attention_kernel,
        out_shape=jax.ShapeDtypeStruct((OUTER, 2 * HD + EXTRA, QC), jnp.bfloat16),
        grid=(OUTER // PER,),
        in_specs=[
            pl.BlockSpec(memory_space=pltpu.SMEM),
            pl.BlockSpec(memory_space=pltpu.SMEM),
            pl.BlockSpec((PER, ROWS, HEADS * HD), lambda i: (i, 0, 0)),
            *[pl.BlockSpec((2 * ROWS, HD), lambda i: (0, 0)) for _ in range(INNER)],
            pl.BlockSpec((PER, 16, n_keys), lambda i: (i, 0, 0)),
        ],
        out_specs=pl.BlockSpec((PER, 2 * HD + EXTRA, QC), lambda i: (i, 0, 0)),
        scratch_shapes=[
            pltpu.VMEM((INNER, 2, CH, 2 * HD), jnp.bfloat16),
            pltpu.VMEM((n_keys + CH, 2 * HD), jnp.bfloat16),
            pltpu.VMEM((HD, n_keys + CH), jnp.bfloat16),
            pltpu.VMEM((HD, n_keys), jnp.bfloat16),
            pltpu.VMEM((HD, n_keys), jnp.bfloat16),
        ],
        compiler_params=pltpu.CompilerParams(dimension_semantics=("arbitrary",)),
        cost_estimate=pl.CostEstimate(flops=8 * 10**9, bytes_accessed=6 * 10**6, transcendentals=5 * 10**6),
        name="partial_attention",
    )(own, sel, q_all, *kv, late)


def combine_kernel(part_ref, out_ref):
    halves = []
    for half in range(2):
        at = 2 * HD + 3 * half
        lse = []
        for o in range(OUTER):
            terms = part_ref[o, 2 * HD :, :].astype(jnp.float32)[3 * half : 3 * half + 3]
            lse.append(terms[0:1] + terms[1:2] + terms[2:3])
        top = lse[0]
        for o in range(1, OUTER):
            top = jnp.maximum(top, lse[o])
        total = jnp.zeros_like(top)
        acc = jnp.zeros((HD, QC), jnp.float32)
        for o in range(OUTER):
            w = jnp.exp2(lse[o] - top)
            total = total + w
            acc = acc + w * part_ref[o, half * HD : (half + 1) * HD, :].astype(jnp.float32)
        mixed = (acc * (1.0 / total)).T
        halves.append(jnp.concatenate([mixed[h * CH : (h + 1) * CH] for h in range(HEADS)], axis=1))
    out_ref[...] = jnp.concatenate(halves, axis=0).astype(jnp.bfloat16)


def combine(parts):
    return pl.pallas_call(
        combine_kernel,
        out_shape=jax.ShapeDtypeStruct((ROWS, HEADS * HD), jnp.bfloat16),
        in_specs=[pl.BlockSpec(memory_space=pltpu.VMEM)],
        out_specs=pl.BlockSpec(memory_space=pltpu.VMEM),
        cost_estimate=pl.CostEstimate(flops=10**8, bytes_accessed=24 * 10**5, transcendentals=0),
        name="combine",
    )(parts)


def project_kernel(place_ref, x_ref, y_ref, w_ref, v_ref, *outs):
    step = pl.program_id(0)
    got = dot(x_ref[...], w_ref[...], ((1,), (0,))) + dot(y_ref[...], v_ref[...], ((1,), (0,)))
    got = got.astype(jnp.bfloat16)
    for n, out in enumerate(outs):

        @pl.when(step == n)
        def _():
            out[...] = got


def project(place, x, y, w_own, w_other, hops):
    def target(i, place_ref):
        hop = jnp.int32(hops[-1])
        for n in range(len(hops) - 1):
            hop = jnp.where(i // 2 == n, jnp.int32(hops[n]), hop)
        return lax.rem(place_ref[0] + hop, ZHI)

    def own_block(i, place_ref):
        return (0, (2 * target(i, place_ref) + place_ref[1]) * 2 + lax.rem(i, 2))

    count = 2 * len(hops)
    width = x.shape[1]
    return pl.pallas_call(
        project_kernel,
        out_shape=[jax.ShapeDtypeStruct((ROWS, HALF), jnp.bfloat16)] * count,
        grid_spec=pltpu.PrefetchScalarGridSpec(
            num_scalar_prefetch=1,
            grid=(count,),
            in_specs=[
                pl.BlockSpec((ROWS, width), lambda i, p: (0, 0)),
                pl.BlockSpec((ROWS, width), lambda i, p: (0, 0)),
                pl.BlockSpec((width, HALF), own_block),
                pl.BlockSpec((width, HALF), own_block),
            ],
            out_specs=[pl.BlockSpec((ROWS, HALF), lambda i, p: (0, 0))] * count,
        ),
        compiler_params=pltpu.CompilerParams(dimension_semantics=("arbitrary",)),
        cost_estimate=pl.CostEstimate(
            flops=2 * ROWS * 2 * width * HALF * count,
            bytes_accessed=2 * width * HALF * count * 2,
            transcendentals=0,
        ),
        name="project",
    )(place, x, y, w_own, w_other)


def added(*terms):
    return sum(t.astype(jnp.float32) for t in terms).astype(jnp.bfloat16)


def shards(queries, keys, values, stretch_order, w_out):
    o = lax.axis_index("outer")
    i = lax.axis_index("inner")
    t = lax.axis_index("tensor")
    z, core = t // 2, t % 2

    kv_own = jnp.concatenate([keys, values], axis=0)
    q_many = jnp.broadcast_to(queries[None], (OUTER,) + queries.shape)
    kv = [kv_own]
    for s in range(1, INNER):
        kv.append(lax.ppermute(kv_own, "inner", [((n + s) % INNER, n) for n in range(INNER)]))
    q_all = lax.all_to_all(q_many, "outer", 0, 0, tiled=True)

    early = stretch_order.reshape(OUTER, INNER, 2)[:, :, 0]
    j = lax.dynamic_index_in_dim(early, i, 1, keepdims=False)
    k_here = lax.dynamic_index_in_dim(early, o, 0, keepdims=False)
    k_here = lax.dynamic_slice_in_dim(jnp.concatenate([k_here, k_here]), i, INNER)
    late = (k_here[None, :] > j[:, None]).astype(jnp.int32)
    late_rows = jnp.broadcast_to(
        jnp.repeat(late, CH, axis=1).astype(jnp.bfloat16)[:, None, :], (OUTER, 16, INNER * CH)
    )

    q_all, kv, w_send = lax.optimization_barrier((q_all, kv, w_out))
    swap = [(n, n ^ 1) for n in range(2 * ZHI)]
    w_other = lax.ppermute(w_send, "tensor", swap)

    parts = partial_attention(o.reshape(1), late.reshape(-1), q_all, kv, late_rows)
    parts = lax.all_to_all(parts, "outer", 0, 0, tiled=True)
    attn = combine(parts)
    attn_other = lax.ppermute(attn, "tensor", swap)

    place = jnp.stack([z, core]).astype(jnp.int32)
    up = [(n, (n + 2) % (2 * ZHI)) for n in range(2 * ZHI)]
    down = [(n, (n - 2) % (2 * ZHI)) for n in range(2 * ZHI)]
    far_a, far_b = project(place, attn, attn_other, w_out, w_other, (2,))
    relay_a = lax.ppermute(far_a, "tensor", up)
    relay_b = lax.ppermute(far_b, "tensor", down)
    up_a, up_b, down_a, down_b, own_a, own_b = project(
        place, attn, attn_other, w_out, w_other, (1, 3, 0)
    )
    plain_b = lax.ppermute(up_b, "tensor", up)
    plain_a = lax.ppermute(down_a, "tensor", down)
    sum_a = lax.ppermute(added(up_a, relay_a), "tensor", up)
    sum_b = lax.ppermute(added(down_b, relay_b), "tensor", down)
    return jnp.concatenate([added(own_a, plain_a, sum_a), added(own_b, plain_b, sum_b)], axis=1)


def solution(mesh):
    placed = (
        P(("outer", "inner"), "tensor"),
        P(("outer", "inner"), "tensor"),
        P(("outer", "inner"), "tensor"),
        P(),
        P("tensor", None),
    )
    return jax.shard_map(
        shards,
        mesh=mesh,
        in_specs=placed,
        out_specs=P(("outer", "inner"), "tensor"),
        check_vma=False,
    )
```

```python
import math

import jax
import jax.numpy as jnp
from jax import lax
from jax.experimental import pallas as pl
from jax.experimental.pallas import tpu as pltpu
from jax.sharding import PartitionSpec as P


HD = 128
HEADS = 4
CH = 64
ROWS = 2 * CH
OUTER = 16
INNER = 8
FAR = 4
ZHI = 4
QC = HEADS * CH
EXTRA = 16
NEG = -1e30
COEF = math.log2(math.e) / math.sqrt(HD)
PER = 2
HALF = 512


def dot(a, b, dims):
    return lax.dot_general(a, b, (dims, ((), ())), preferred_element_type=jnp.float32)


def three_terms(x):
    hi = x.astype(jnp.bfloat16)
    rest = x - hi.astype(jnp.float32)
    mid = rest.astype(jnp.bfloat16)
    low = (rest - mid.astype(jnp.float32)).astype(jnp.bfloat16)
    return hi.astype(jnp.float32), mid.astype(jnp.float32), low.astype(jnp.float32)


def attention_kernel(own_ref, sel_ref, q_ref, *refs):
    pairs = refs[:FAR]
    late_ref, oe_ref, ol_ref, pick, dense, vt_dense, vt_e, vt_l = refs[FAR:]

    def rows_of(s, at):
        first = (s // FAR) * 2 * ROWS + at
        return pairs[s % FAR][first : first + CH, :]

    step = pl.program_id(0)
    keys_dense = INNER * CH

    @pl.when(step == 0)
    def _():
        zero = jnp.zeros((CH, HD), jnp.bfloat16)
        for s in range(INNER):
            k_e = rows_of(s, 0)
            k_l = rows_of(s, CH)
            pick[s, 0] = jnp.concatenate([k_e, zero], axis=1)
            pick[s, 1] = jnp.concatenate([zero, k_l], axis=1)
            dense[s * CH : (s + 1) * CH, :] = jnp.concatenate([zero, k_e], axis=1)
        dense[keys_dense:, :] = jnp.concatenate([zero, rows_of(0, CH)], axis=1)
        v_e = jnp.concatenate([rows_of(s, ROWS) for s in range(INNER)], axis=0)
        v_l = jnp.concatenate([rows_of(s, ROWS + CH) for s in range(INNER)], axis=0)
        t_e = v_e.astype(jnp.float32).T.astype(jnp.bfloat16)
        t_l = v_l.astype(jnp.float32).T.astype(jnp.bfloat16)
        vt_e[...] = t_e
        vt_l[...] = t_l
        vt_dense[:, :keys_dense] = t_e
        vt_dense[:, keys_dense:] = t_l[:, :CH]

    key_at = lax.broadcasted_iota(jnp.int32, (CH, QC), 0)
    query_at = lax.broadcasted_iota(jnp.int32, (CH, QC), 1) % CH
    causal = key_at <= query_at

    for p in range(PER):
        a = step * PER + p
        own = a == own_ref[0]
        q = q_ref[p]
        stacked = [
            jnp.concatenate([q[r : r + CH, h * HD : (h + 1) * HD] for h in range(HEADS)], axis=0)
            for r in (0, CH)
        ]
        q_cat = jnp.concatenate(stacked, axis=1)
        s_dense = dot(dense[...], q_cat, ((1,), (1,)))
        late = [sel_ref[a * INNER + s] > 0 for s in range(INNER)]
        chosen = jnp.concatenate([pick[s, sel_ref[a * INNER + s]] for s in range(INNER)], axis=0)
        s_sel = dot(chosen, q_cat, ((1,), (1,)))
        keep = jnp.where(own, 1, 0)
        s_first = jnp.where(jnp.logical_or(causal, keep == 0), s_sel[:CH], NEG)
        s_extra = jnp.where(jnp.logical_and(causal, keep == 1), s_dense[keys_dense:], NEG)
        blocks = [s_first] + [s_sel[s * CH : (s + 1) * CH] for s in range(1, INNER)]
        tops = [jnp.max(b, axis=0, keepdims=True) for b in blocks]
        m_e = jnp.full((1, QC), NEG, jnp.float32)
        m_l = jnp.maximum(
            jnp.max(s_dense[:keys_dense], axis=0, keepdims=True),
            jnp.max(s_extra, axis=0, keepdims=True),
        )
        for s in range(INNER):
            m_e = jnp.maximum(m_e, jnp.where(late[s], NEG, tops[s]))
            m_l = jnp.maximum(m_l, jnp.where(late[s], tops[s], NEG))
        p_dense = jnp.exp2((s_dense[:keys_dense] - m_l) * COEF)
        p_extra = jnp.exp2((s_extra - m_l) * COEF)
        l_l = jnp.sum(p_dense, axis=0, keepdims=True) + jnp.sum(p_extra, axis=0, keepdims=True)
        l_e = jnp.zeros((1, QC), jnp.float32)
        weights = []
        for s in range(INNER):
            w = jnp.exp2((blocks[s] - jnp.where(late[s], m_l, m_e)) * COEF)
            part = jnp.sum(w, axis=0, keepdims=True)
            l_e = l_e + jnp.where(late[s], 0.0, part)
            l_l = l_l + jnp.where(late[s], part, 0.0)
            weights.append(w.astype(jnp.bfloat16))
        w_sel = jnp.concatenate(weights, axis=0)
        w_dense = jnp.concatenate([p_dense.astype(jnp.bfloat16), p_extra.astype(jnp.bfloat16)], axis=0)
        is_late = late_ref[p, 0:1, :]
        v_sel = jnp.concatenate([vt_e[...] * (1 - is_late), vt_l[...] * is_late], axis=0)
        o_sel = dot(v_sel, w_sel, ((1,), (0,)))
        o_e = o_sel[:HD]
        o_l = o_sel[HD:] + dot(vt_dense[...], w_dense, ((1,), (0,)))
        some = l_e > 0.0
        inv_e = jnp.where(some, 1.0 / jnp.where(some, l_e, 1.0), 0.0)
        lse_e = jnp.where(some, m_e * COEF + jnp.log2(jnp.where(some, l_e, 1.0)), NEG)
        lse_l = m_l * COEF + jnp.log2(l_l)
        for ref, o_t, inv, lse in ((oe_ref, o_e, inv_e, lse_e), (ol_ref, o_l, 1.0 / l_l, lse_l)):
            ref[p, :HD, :] = (o_t * inv).astype(jnp.bfloat16)
            rows = list(three_terms(lse)) + [jnp.zeros((EXTRA - 3, QC), jnp.float32)]
            ref[p, HD:, :] = jnp.concatenate(rows, axis=0).astype(jnp.bfloat16)


def partial_attention(own, sel, q_all, kv, late):
    n_keys = INNER * CH
    return pl.pallas_call(
        attention_kernel,
        out_shape=[jax.ShapeDtypeStruct((OUTER, HD + EXTRA, QC), jnp.bfloat16)] * 2,
        grid=(OUTER // PER,),
        in_specs=[
            pl.BlockSpec(memory_space=pltpu.SMEM),
            pl.BlockSpec(memory_space=pltpu.SMEM),
            pl.BlockSpec((PER, ROWS, HEADS * HD), lambda i: (i, 0, 0)),
            *[pl.BlockSpec((4 * ROWS, HD), lambda i: (0, 0)) for _ in range(FAR)],
            pl.BlockSpec((PER, 16, n_keys), lambda i: (i, 0, 0)),
        ],
        out_specs=[pl.BlockSpec((PER, HD + EXTRA, QC), lambda i: (i, 0, 0))] * 2,
        scratch_shapes=[
            pltpu.VMEM((INNER, 2, CH, 2 * HD), jnp.bfloat16),
            pltpu.VMEM((n_keys + CH, 2 * HD), jnp.bfloat16),
            pltpu.VMEM((HD, n_keys + CH), jnp.bfloat16),
            pltpu.VMEM((HD, n_keys), jnp.bfloat16),
            pltpu.VMEM((HD, n_keys), jnp.bfloat16),
        ],
        compiler_params=pltpu.CompilerParams(dimension_semantics=("arbitrary",)),
        cost_estimate=pl.CostEstimate(flops=8 * 10**9, bytes_accessed=6 * 10**6, transcendentals=5 * 10**6),
        name="partial_attention",
    )(own, sel, q_all, *kv, late)


def combine_kernel(part_ref, out_ref):
    lse = []
    for o in range(OUTER):
        terms = part_ref[o, HD:, :].astype(jnp.float32)
        lse.append(terms[0:1] + terms[1:2] + terms[2:3])
    top = lse[0]
    for o in range(1, OUTER):
        top = jnp.maximum(top, lse[o])
    total = jnp.zeros_like(top)
    acc = jnp.zeros((HD, QC), jnp.float32)
    for o in range(OUTER):
        w = jnp.exp2(lse[o] - top)
        total = total + w
        acc = acc + w * part_ref[o, :HD, :].astype(jnp.float32)
    mixed = (acc * (1.0 / total)).T
    heads = [mixed[h * CH : (h + 1) * CH] for h in range(HEADS)]
    out_ref[...] = jnp.concatenate(heads, axis=1).astype(jnp.bfloat16)


def combine(parts):
    return pl.pallas_call(
        combine_kernel,
        out_shape=jax.ShapeDtypeStruct((CH, HEADS * HD), jnp.bfloat16),
        in_specs=[pl.BlockSpec(memory_space=pltpu.VMEM)],
        out_specs=pl.BlockSpec(memory_space=pltpu.VMEM),
        cost_estimate=pl.CostEstimate(flops=10**8, bytes_accessed=12 * 10**5, transcendentals=0),
        name="combine",
    )(parts)


def project_kernel(place_ref, x_ref, y_ref, w_ref, v_ref, *outs):
    step = pl.program_id(0)
    got = dot(x_ref[...], w_ref[...], ((1,), (0,))) + dot(y_ref[...], v_ref[...], ((1,), (0,)))
    got = got.astype(jnp.bfloat16)
    for n, out in enumerate(outs):

        @pl.when(step == n)
        def _():
            out[...] = got


def project(place, x, y, w_own, w_other, hops, width):
    cuts = 2 * HALF // width

    def block(i, place_ref):
        hop = jnp.int32(hops[-1])
        for n in range(len(hops) - 1):
            hop = jnp.where(i // cuts == n, jnp.int32(hops[n]), hop)
        to = lax.rem(place_ref[0] + hop, ZHI)
        return (0, (2 * to + place_ref[1]) * cuts + lax.rem(i, cuts))

    rows, depth = x.shape
    count = cuts * len(hops)
    return pl.pallas_call(
        project_kernel,
        out_shape=[jax.ShapeDtypeStruct((rows, width), jnp.bfloat16)] * count,
        grid_spec=pltpu.PrefetchScalarGridSpec(
            num_scalar_prefetch=1,
            grid=(count,),
            in_specs=[
                pl.BlockSpec((rows, depth), lambda i, p: (0, 0)),
                pl.BlockSpec((rows, depth), lambda i, p: (0, 0)),
                pl.BlockSpec((depth, width), block),
                pl.BlockSpec((depth, width), block),
            ],
            out_specs=[pl.BlockSpec((rows, width), lambda i, p: (0, 0))] * count,
        ),
        compiler_params=pltpu.CompilerParams(dimension_semantics=("arbitrary",)),
        cost_estimate=pl.CostEstimate(
            flops=10 * 2 * rows * 2 * depth * width * count,
            bytes_accessed=2 * depth * width * count * 2,
            transcendentals=0,
        ),
        name="project",
    )(place, x, y, w_own, w_other)


def added(*terms):
    return sum(t.astype(jnp.float32) for t in terms).astype(jnp.bfloat16)


def xor_to(axis, size, mask, x):
    return lax.ppermute(x, axis, [(n, n ^ mask) for n in range(size)])


def shards(queries, keys, values, stretch_order, w_out):
    o = lax.axis_index("outer")
    i = lax.axis_index("inner")
    t = lax.axis_index("tensor")
    z, core = t // 2, t % 2
    place = jnp.stack([z, core]).astype(jnp.int32)

    q_many = jnp.broadcast_to(queries[None], (OUTER,) + queries.shape)
    q_all = lax.all_to_all(q_many, "outer", 0, 0, tiled=True)
    early = stretch_order.reshape(OUTER, INNER, 2)[:, :, 0]
    j = lax.dynamic_index_in_dim(early, i, 1, keepdims=False)
    k_row = lax.dynamic_index_in_dim(early, o, 0, keepdims=False)
    slots = jnp.arange(INNER, dtype=jnp.int32)
    hit = (slots[:, None] ^ i) == slots[None, :]
    k_here = jnp.sum(jnp.where(hit, k_row[None, :], 0), axis=1)
    late = (k_here[None, :] > j[:, None]).astype(jnp.int32)
    late_rows = jnp.broadcast_to(
        jnp.repeat(late, CH, axis=1).astype(jnp.bfloat16)[:, None, :], (OUTER, 16, INNER * CH)
    )

    kv_own = jnp.concatenate([keys, values], axis=0)
    kv_own = jnp.concatenate([kv_own, xor_to("inner", INNER, FAR, kv_own)], axis=0)
    kv_own, late, late_rows, place = lax.optimization_barrier((kv_own, late, late_rows, place))
    kv = [kv_own] + [xor_to("inner", INNER, s, kv_own) for s in range(1, FAR)]

    q_all, kv, w_send = lax.optimization_barrier((q_all, kv, w_out))
    w_other = xor_to("tensor", 2 * ZHI, 1, w_send)

    part_e, part_l = partial_attention(o.reshape(1), late.reshape(-1), q_all, kv, late_rows)
    part_e = lax.all_to_all(part_e, "outer", 0, 0, tiled=True)
    part_e, part_l = lax.optimization_barrier((part_e, part_l))
    part_l = lax.all_to_all(part_l, "outer", 0, 0, tiled=True)

    up = [(n, (n + 2) % (2 * ZHI)) for n in range(2 * ZHI)]
    down = [(n, (n - 2) % (2 * ZHI)) for n in range(2 * ZHI)]
    results = []
    for half in range(2):
        x = combine(part_l if half else part_e)
        y = xor_to("tensor", 2 * ZHI, 1, x)
        far_a, far_b = project(place, x, y, w_out, w_other, (2,), HALF)
        relay_a = lax.ppermute(far_a, "tensor", up)
        relay_b = lax.ppermute(far_b, "tensor", down)
        to_up, to_down, mine = project(place, x, y, w_out, w_other, (1, 3, 0), 2 * HALF)
        zero = jnp.zeros((), jnp.bfloat16)
        to_up = added(to_up, lax.pad(relay_a, zero, ((0, 0, 0), (0, HALF, 0))))
        to_down = added(to_down, lax.pad(relay_b, zero, ((0, 0, 0), (HALF, 0, 0))))
        if half == 0:
            part_l, to_up, to_down = lax.optimization_barrier((part_l, to_up, to_down))
        below = lax.ppermute(to_up, "tensor", up)
        above = lax.ppermute(to_down, "tensor", down)
        results.append(added(mine, below, above))
    return jnp.concatenate(results, axis=0)


def solution(mesh):
    placed = (
        P(("outer", "inner"), "tensor"),
        P(("outer", "inner"), "tensor"),
        P(("outer", "inner"), "tensor"),
        P(),
        P("tensor", None),
    )
    return jax.shard_map(
        shards,
        mesh=mesh,
        in_specs=placed,
        out_specs=P(("outer", "inner"), "tensor"),
        check_vma=False,
    )
```

```python
import math

import jax
import jax.numpy as jnp
from jax import lax
from jax.experimental import pallas as pl
from jax.experimental.pallas import tpu as pltpu
from jax.sharding import PartitionSpec as P


HD = 128
HEADS = 4
CH = 64
ROWS = 2 * CH
OUTER = 16
INNER = 8
FAR = 4
ZHI = 4
GROUP = 2
QC = GROUP * CH
EXTRA = 16
NEG = -1e30
COEF = math.log2(math.e) / math.sqrt(HD)
PER = 4
HALF = 512


def dot(a, b, dims):
    return lax.dot_general(a, b, (dims, ((), ())), preferred_element_type=jnp.float32)


def three_terms(x):
    hi = x.astype(jnp.bfloat16)
    rest = x - hi.astype(jnp.float32)
    mid = rest.astype(jnp.bfloat16)
    low = (rest - mid.astype(jnp.float32)).astype(jnp.bfloat16)
    return hi.astype(jnp.float32), mid.astype(jnp.float32), low.astype(jnp.float32)


def attention_kernel(own_ref, sel_ref, q_ref, *refs):
    pairs = refs[:FAR]
    late_ref, out_ref, pick, dense, vt_dense, vt_e, vt_l = refs[FAR:]

    def rows_of(s, at):
        first = (s // FAR) * 2 * ROWS + at
        return pairs[s % FAR][first : first + CH, :]

    step = pl.program_id(0)
    keys_dense = INNER * CH

    @pl.when(step == 0)
    def _():
        zero = jnp.zeros((CH, HD), jnp.bfloat16)
        for s in range(INNER):
            k_e = rows_of(s, 0)
            k_l = rows_of(s, CH)
            pick[s, 0] = jnp.concatenate([k_e, zero], axis=1)
            pick[s, 1] = jnp.concatenate([zero, k_l], axis=1)
            dense[s * CH : (s + 1) * CH, :] = jnp.concatenate([zero, k_e], axis=1)
        dense[keys_dense:, :] = jnp.concatenate([zero, rows_of(0, CH)], axis=1)
        v_e = jnp.concatenate([rows_of(s, ROWS) for s in range(INNER)], axis=0)
        v_l = jnp.concatenate([rows_of(s, ROWS + CH) for s in range(INNER)], axis=0)
        t_e = v_e.astype(jnp.float32).T.astype(jnp.bfloat16)
        t_l = v_l.astype(jnp.float32).T.astype(jnp.bfloat16)
        vt_e[...] = t_e
        vt_l[...] = t_l
        vt_dense[:, :keys_dense] = t_e
        vt_dense[:, keys_dense:] = t_l[:, :CH]

    key_at = lax.broadcasted_iota(jnp.int32, (CH, QC), 0)
    query_at = lax.broadcasted_iota(jnp.int32, (CH, QC), 1) % CH
    causal = key_at <= query_at

    for p in range(PER):
        a = step * PER + p
        own = a == own_ref[0]
        q = q_ref[p]
        stacked = [
            jnp.concatenate([q[r : r + CH, h * HD : (h + 1) * HD] for h in range(GROUP)], axis=0)
            for r in (0, CH)
        ]
        q_cat = jnp.concatenate(stacked, axis=1)
        s_dense = dot(dense[...], q_cat, ((1,), (1,)))
        late = [sel_ref[a * INNER + s] > 0 for s in range(INNER)]
        chosen = jnp.concatenate([pick[s, sel_ref[a * INNER + s]] for s in range(INNER)], axis=0)
        s_sel = dot(chosen, q_cat, ((1,), (1,)))
        keep = jnp.where(own, 1, 0)
        s_first = jnp.where(jnp.logical_or(causal, keep == 0), s_sel[:CH], NEG)
        s_extra = jnp.where(jnp.logical_and(causal, keep == 1), s_dense[keys_dense:], NEG)
        blocks = [s_first] + [s_sel[s * CH : (s + 1) * CH] for s in range(1, INNER)]
        tops = [jnp.max(b, axis=0, keepdims=True) for b in blocks]
        m_e = jnp.full((1, QC), NEG, jnp.float32)
        m_l = jnp.maximum(
            jnp.max(s_dense[:keys_dense], axis=0, keepdims=True),
            jnp.max(s_extra, axis=0, keepdims=True),
        )
        for s in range(INNER):
            m_e = jnp.maximum(m_e, jnp.where(late[s], NEG, tops[s]))
            m_l = jnp.maximum(m_l, jnp.where(late[s], tops[s], NEG))
        p_dense = jnp.exp2((s_dense[:keys_dense] - m_l) * COEF)
        p_extra = jnp.exp2((s_extra - m_l) * COEF)
        l_l = jnp.sum(p_dense, axis=0, keepdims=True) + jnp.sum(p_extra, axis=0, keepdims=True)
        l_e = jnp.zeros((1, QC), jnp.float32)
        weights = []
        for s in range(INNER):
            w = jnp.exp2((blocks[s] - jnp.where(late[s], m_l, m_e)) * COEF)
            part = jnp.sum(w, axis=0, keepdims=True)
            l_e = l_e + jnp.where(late[s], 0.0, part)
            l_l = l_l + jnp.where(late[s], part, 0.0)
            weights.append(w.astype(jnp.bfloat16))
        w_sel = jnp.concatenate(weights, axis=0)
        w_dense = jnp.concatenate([p_dense.astype(jnp.bfloat16), p_extra.astype(jnp.bfloat16)], axis=0)
        is_late = late_ref[p, 0:1, :]
        v_sel = jnp.concatenate([vt_e[...] * (1 - is_late), vt_l[...] * is_late], axis=0)
        o_sel = dot(v_sel, w_sel, ((1,), (0,)))
        o_e = o_sel[:HD]
        o_l = o_sel[HD:] + dot(vt_dense[...], w_dense, ((1,), (0,)))
        some = l_e > 0.0
        inv_e = jnp.where(some, 1.0 / jnp.where(some, l_e, 1.0), 0.0)
        lse_e = jnp.where(some, m_e * COEF + jnp.log2(jnp.where(some, l_e, 1.0)), NEG)
        lse_l = m_l * COEF + jnp.log2(l_l)
        for at, o_t, inv, lse in ((0, o_e, inv_e, lse_e), (QC, o_l, 1.0 / l_l, lse_l)):
            rows = list(three_terms(lse)) + [jnp.zeros((EXTRA - 3, QC), jnp.float32)]
            out_ref[p, :HD, at : at + QC] = (o_t * inv).astype(jnp.bfloat16)
            out_ref[p, HD:, at : at + QC] = jnp.concatenate(rows, axis=0).astype(jnp.bfloat16)


def partial_attention(own, sel, q_all, kv, late, group):
    n_keys = INNER * CH
    return pl.pallas_call(
        attention_kernel,
        out_shape=jax.ShapeDtypeStruct((OUTER, HD + EXTRA, 2 * QC), jnp.bfloat16),
        grid=(OUTER // PER,),
        in_specs=[
            pl.BlockSpec(memory_space=pltpu.SMEM),
            pl.BlockSpec(memory_space=pltpu.SMEM),
            pl.BlockSpec((PER, ROWS, GROUP * HD), lambda i: (i, 0, group)),
            *[pl.BlockSpec((4 * ROWS, HD), lambda i: (0, 0)) for _ in range(FAR)],
            pl.BlockSpec((PER, 16, n_keys), lambda i: (i, 0, 0)),
        ],
        out_specs=pl.BlockSpec((PER, HD + EXTRA, 2 * QC), lambda i: (i, 0, 0)),
        scratch_shapes=[
            pltpu.VMEM((INNER, 2, CH, 2 * HD), jnp.bfloat16),
            pltpu.VMEM((n_keys + CH, 2 * HD), jnp.bfloat16),
            pltpu.VMEM((HD, n_keys + CH), jnp.bfloat16),
            pltpu.VMEM((HD, n_keys), jnp.bfloat16),
            pltpu.VMEM((HD, n_keys), jnp.bfloat16),
        ],
        compiler_params=pltpu.CompilerParams(dimension_semantics=("arbitrary",)),
        cost_estimate=pl.CostEstimate(flops=4 * 10**9, bytes_accessed=3 * 10**6, transcendentals=2 * 10**6),
        name="partial_attention",
    )(own, sel, q_all, *kv, late)


def combine_kernel(part_ref, out_ref):
    lse = []
    for o in range(OUTER):
        terms = part_ref[o, HD:, :].astype(jnp.float32)
        lse.append(terms[0:1] + terms[1:2] + terms[2:3])
    top = lse[0]
    for o in range(1, OUTER):
        top = jnp.maximum(top, lse[o])
    total = jnp.zeros_like(top)
    acc = jnp.zeros((HD, 2 * QC), jnp.float32)
    for o in range(OUTER):
        w = jnp.exp2(lse[o] - top)
        total = total + w
        acc = acc + w * part_ref[o, :HD, :].astype(jnp.float32)
    mixed = (acc * (1.0 / total)).T
    halves = []
    for at in (0, QC):
        heads = [mixed[at + h * CH : at + (h + 1) * CH] for h in range(GROUP)]
        halves.append(jnp.concatenate(heads, axis=1))
    out_ref[...] = jnp.concatenate(halves, axis=0).astype(jnp.bfloat16)


def combine(parts):
    return pl.pallas_call(
        combine_kernel,
        out_shape=jax.ShapeDtypeStruct((ROWS, GROUP * HD), jnp.bfloat16),
        in_specs=[pl.BlockSpec(memory_space=pltpu.VMEM)],
        out_specs=pl.BlockSpec(memory_space=pltpu.VMEM),
        cost_estimate=pl.CostEstimate(flops=10**8, bytes_accessed=12 * 10**5, transcendentals=0),
        name="combine",
    )(parts)


def project_kernel(place_ref, x0_ref, x1_ref, y0_ref, y1_ref, w_ref, v_ref, *outs):
    step = pl.program_id(0)
    x = jnp.concatenate([x0_ref[...], x1_ref[...]], axis=1)
    y = jnp.concatenate([y0_ref[...], y1_ref[...]], axis=1)
    got = dot(x, w_ref[...], ((1,), (0,))) + dot(y, v_ref[...], ((1,), (0,)))
    got = got.astype(jnp.bfloat16)
    for n, out in enumerate(outs):

        @pl.when(step == n)
        def _():
            out[...] = got


def project(place, x, y, w_own, w_other, hops, width):
    cuts = 2 * HALF // width

    def block(i, place_ref):
        hop = jnp.int32(hops[-1])
        for n in range(len(hops) - 1):
            hop = jnp.where(i // cuts == n, jnp.int32(hops[n]), hop)
        to = lax.rem(place_ref[0] + hop, ZHI)
        return (0, (2 * to + place_ref[1]) * cuts + lax.rem(i, cuts))

    rows, depth = x[0].shape[0], 2 * x[0].shape[1]
    count = cuts * len(hops)
    return pl.pallas_call(
        project_kernel,
        out_shape=[jax.ShapeDtypeStruct((rows, width), jnp.bfloat16)] * count,
        grid_spec=pltpu.PrefetchScalarGridSpec(
            num_scalar_prefetch=1,
            grid=(count,),
            in_specs=[
                *[pl.BlockSpec((rows, depth // 2), lambda i, p: (0, 0)) for _ in range(4)],
                pl.BlockSpec((depth, width), block),
                pl.BlockSpec((depth, width), block),
            ],
            out_specs=[pl.BlockSpec((rows, width), lambda i, p: (0, 0))] * count,
        ),
        compiler_params=pltpu.CompilerParams(dimension_semantics=("arbitrary",)),
        cost_estimate=pl.CostEstimate(
            flops=10 * 2 * rows * 2 * depth * width * count,
            bytes_accessed=2 * depth * width * count * 2,
            transcendentals=0,
        ),
        name="project",
    )(place, *x, *y, w_own, w_other)


def added(*terms):
    return sum(t.astype(jnp.float32) for t in terms).astype(jnp.bfloat16)


def xor_to(axis, size, mask, x):
    return lax.ppermute(x, axis, [(n, n ^ mask) for n in range(size)])


def shards(queries, keys, values, stretch_order, w_out):
    o = lax.axis_index("outer")
    i = lax.axis_index("inner")
    t = lax.axis_index("tensor")
    z, core = t // 2, t % 2
    place = jnp.stack([z, core]).astype(jnp.int32)

    early = stretch_order.reshape(OUTER, INNER, 2)[:, :, 0]
    j = lax.dynamic_index_in_dim(early, i, 1, keepdims=False)
    k_row = lax.dynamic_index_in_dim(early, o, 0, keepdims=False)
    slots = jnp.arange(INNER, dtype=jnp.int32)
    hit = (slots[:, None] ^ i) == slots[None, :]
    k_here = jnp.sum(jnp.where(hit, k_row[None, :], 0), axis=1)
    late = (k_here[None, :] > j[:, None]).astype(jnp.int32)
    late_rows = jnp.broadcast_to(
        jnp.repeat(late, CH, axis=1).astype(jnp.bfloat16)[:, None, :], (OUTER, 16, INNER * CH)
    )

    kv_own = jnp.concatenate([keys, values], axis=0)
    kv_far = xor_to("inner", INNER, FAR, kv_own)
    q_many = jnp.broadcast_to(queries[None], (OUTER,) + queries.shape)
    q_all = lax.all_to_all(q_many, "outer", 0, 0, tiled=True)
    kv_own = jnp.concatenate([kv_own, kv_far], axis=0)
    kv_own, late, late_rows, place = lax.optimization_barrier((kv_own, late, late_rows, place))
    kv = [kv_own] + [xor_to("inner", INNER, s, kv_own) for s in range(1, FAR)]

    q_all, kv, w_send = lax.optimization_barrier((q_all, kv, w_out))
    w_other = xor_to("tensor", 2 * ZHI, 1, w_send)

    own, sel = o.reshape(1), late.reshape(-1)
    parts = []
    for g in range(HEADS // GROUP):
        part = partial_attention(own, sel, q_all, kv, late_rows, g)
        parts.append(lax.all_to_all(part, "outer", 0, 0, tiled=True))
    x, y = [], []
    for g in range(HEADS // GROUP):
        x.append(combine(parts[g]))
        y.append(xor_to("tensor", 2 * ZHI, 1, x[-1]))

    up = [(n, (n + 2) % (2 * ZHI)) for n in range(2 * ZHI)]
    down = [(n, (n - 2) % (2 * ZHI)) for n in range(2 * ZHI)]
    far_a, far_b = project(place, x, y, w_out, w_other, (2,), HALF)
    relay_a = lax.ppermute(far_a, "tensor", up)
    relay_b = lax.ppermute(far_b, "tensor", down)
    up_a, up_b, down_a, down_b, own_a, own_b = project(place, x, y, w_out, w_other, (1, 3, 0), HALF)
    plain_b = lax.ppermute(up_b, "tensor", up)
    plain_a = lax.ppermute(down_a, "tensor", down)
    sum_a = lax.ppermute(added(up_a, relay_a), "tensor", up)
    sum_b = lax.ppermute(added(down_b, relay_b), "tensor", down)
    return jnp.concatenate([added(own_a, plain_a, sum_a), added(own_b, plain_b, sum_b)], axis=1)


def solution(mesh):
    placed = (
        P(("outer", "inner"), "tensor"),
        P(("outer", "inner"), "tensor"),
        P(("outer", "inner"), "tensor"),
        P(),
        P("tensor", None),
    )
    return jax.shard_map(
        shards,
        mesh=mesh,
        in_specs=placed,
        out_specs=P(("outer", "inner"), "tensor"),
        check_vma=False,
    )
```

```python
import math

import jax
import jax.numpy as jnp
from jax import lax
from jax.experimental import pallas as pl
from jax.experimental.pallas import tpu as pltpu
from jax.sharding import PartitionSpec as P


HD = 128
CH = 64
ROWS = 2 * CH
OUTER = 16
INNER = 8
FAR = 4
ZHI = 4
GROUP = 4
QC = GROUP * CH
EXTRA = 16
NEG = -1e30
COEF = math.log2(math.e) / math.sqrt(HD)
PER = 4
OUT = 1024


def dot(a, b, dims):
    return lax.dot_general(a, b, (dims, ((), ())), preferred_element_type=jnp.float32)


def three_terms(x):
    hi = x.astype(jnp.bfloat16)
    rest = x - hi.astype(jnp.float32)
    mid = rest.astype(jnp.bfloat16)
    low = (rest - mid.astype(jnp.float32)).astype(jnp.bfloat16)
    return hi.astype(jnp.float32), mid.astype(jnp.float32), low.astype(jnp.float32)


def attention_kernel(own_ref, sel_ref, q_ref, *refs):
    pairs = refs[:FAR]
    late_ref, out_ref, pick, dense, vt_dense, vt_e, vt_l = refs[FAR:]

    def rows_of(s, at):
        first = (s // FAR) * 2 * ROWS + at
        return pairs[s % FAR][first : first + CH, :]

    step = pl.program_id(0)
    keys_dense = INNER * CH

    @pl.when(step == 0)
    def _():
        zero = jnp.zeros((CH, HD), jnp.bfloat16)
        for s in range(INNER):
            k_e = rows_of(s, 0)
            k_l = rows_of(s, CH)
            pick[s, 0] = jnp.concatenate([k_e, zero], axis=1)
            pick[s, 1] = jnp.concatenate([zero, k_l], axis=1)
            dense[s * CH : (s + 1) * CH, :] = jnp.concatenate([zero, k_e], axis=1)
        dense[keys_dense:, :] = jnp.concatenate([zero, rows_of(0, CH)], axis=1)
        v_e = jnp.concatenate([rows_of(s, ROWS) for s in range(INNER)], axis=0)
        v_l = jnp.concatenate([rows_of(s, ROWS + CH) for s in range(INNER)], axis=0)
        t_e = v_e.astype(jnp.float32).T.astype(jnp.bfloat16)
        t_l = v_l.astype(jnp.float32).T.astype(jnp.bfloat16)
        vt_e[...] = t_e
        vt_l[...] = t_l
        vt_dense[:, :keys_dense] = t_e
        vt_dense[:, keys_dense:] = t_l[:, :CH]

    key_at = lax.broadcasted_iota(jnp.int32, (CH, QC), 0)
    query_at = lax.broadcasted_iota(jnp.int32, (CH, QC), 1) % CH
    causal = key_at <= query_at

    for p in range(PER):
        a = step * PER + p
        own = a == own_ref[0]
        q = q_ref[p]
        stacked = [
            jnp.concatenate([q[r : r + CH, h * HD : (h + 1) * HD] for h in range(GROUP)], axis=0)
            for r in (0, CH)
        ]
        q_cat = jnp.concatenate(stacked, axis=1)
        s_dense = dot(dense[...], q_cat, ((1,), (1,)))
        late = [sel_ref[a * INNER + s] > 0 for s in range(INNER)]
        chosen = jnp.concatenate([pick[s, sel_ref[a * INNER + s]] for s in range(INNER)], axis=0)
        s_sel = dot(chosen, q_cat, ((1,), (1,)))
        keep = jnp.where(own, 1, 0)
        s_first = jnp.where(jnp.logical_or(causal, keep == 0), s_sel[:CH], NEG)
        s_extra = jnp.where(jnp.logical_and(causal, keep == 1), s_dense[keys_dense:], NEG)
        blocks = [s_first] + [s_sel[s * CH : (s + 1) * CH] for s in range(1, INNER)]
        tops = [jnp.max(b, axis=0, keepdims=True) for b in blocks]
        m_e = jnp.full((1, QC), NEG, jnp.float32)
        m_l = jnp.maximum(
            jnp.max(s_dense[:keys_dense], axis=0, keepdims=True),
            jnp.max(s_extra, axis=0, keepdims=True),
        )
        for s in range(INNER):
            m_e = jnp.maximum(m_e, jnp.where(late[s], NEG, tops[s]))
            m_l = jnp.maximum(m_l, jnp.where(late[s], tops[s], NEG))
        p_dense = jnp.exp2((s_dense[:keys_dense] - m_l) * COEF)
        p_extra = jnp.exp2((s_extra - m_l) * COEF)
        l_l = jnp.sum(p_dense, axis=0, keepdims=True) + jnp.sum(p_extra, axis=0, keepdims=True)
        l_e = jnp.zeros((1, QC), jnp.float32)
        weights = []
        for s in range(INNER):
            w = jnp.exp2((blocks[s] - jnp.where(late[s], m_l, m_e)) * COEF)
            part = jnp.sum(w, axis=0, keepdims=True)
            l_e = l_e + jnp.where(late[s], 0.0, part)
            l_l = l_l + jnp.where(late[s], part, 0.0)
            weights.append(w.astype(jnp.bfloat16))
        w_sel = jnp.concatenate(weights, axis=0)
        w_dense = jnp.concatenate([p_dense.astype(jnp.bfloat16), p_extra.astype(jnp.bfloat16)], axis=0)
        is_late = late_ref[p, 0:1, :]
        v_sel = jnp.concatenate([vt_e[...] * (1 - is_late), vt_l[...] * is_late], axis=0)
        o_sel = dot(v_sel, w_sel, ((1,), (0,)))
        o_e = o_sel[:HD]
        o_l = o_sel[HD:] + dot(vt_dense[...], w_dense, ((1,), (0,)))
        some = l_e > 0.0
        inv_e = jnp.where(some, 1.0 / jnp.where(some, l_e, 1.0), 0.0)
        lse_e = jnp.where(some, m_e * COEF + jnp.log2(jnp.where(some, l_e, 1.0)), NEG)
        lse_l = m_l * COEF + jnp.log2(l_l)
        for at, o_t, inv, lse in ((0, o_e, inv_e, lse_e), (QC, o_l, 1.0 / l_l, lse_l)):
            rows = list(three_terms(lse)) + [jnp.zeros((EXTRA - 3, QC), jnp.float32)]
            out_ref[p, :HD, at : at + QC] = (o_t * inv).astype(jnp.bfloat16)
            out_ref[p, HD:, at : at + QC] = jnp.concatenate(rows, axis=0).astype(jnp.bfloat16)


def partial_attention(own, sel, q_all, kv, late, group):
    n_keys = INNER * CH
    return pl.pallas_call(
        attention_kernel,
        out_shape=jax.ShapeDtypeStruct((OUTER, HD + EXTRA, 2 * QC), jnp.bfloat16),
        grid=(OUTER // PER,),
        in_specs=[
            pl.BlockSpec(memory_space=pltpu.SMEM),
            pl.BlockSpec(memory_space=pltpu.SMEM),
            pl.BlockSpec((PER, ROWS, GROUP * HD), lambda i: (i, 0, group)),
            *[pl.BlockSpec((4 * ROWS, HD), lambda i: (0, 0)) for _ in range(FAR)],
            pl.BlockSpec((PER, 16, n_keys), lambda i: (i, 0, 0)),
        ],
        out_specs=pl.BlockSpec((PER, HD + EXTRA, 2 * QC), lambda i: (i, 0, 0)),
        scratch_shapes=[
            pltpu.VMEM((INNER, 2, CH, 2 * HD), jnp.bfloat16),
            pltpu.VMEM((n_keys + CH, 2 * HD), jnp.bfloat16),
            pltpu.VMEM((HD, n_keys + CH), jnp.bfloat16),
            pltpu.VMEM((HD, n_keys), jnp.bfloat16),
            pltpu.VMEM((HD, n_keys), jnp.bfloat16),
        ],
        compiler_params=pltpu.CompilerParams(dimension_semantics=("arbitrary",)),
        cost_estimate=pl.CostEstimate(flops=8 * 10**9, bytes_accessed=6 * 10**6, transcendentals=4 * 10**6),
        name="partial_attention",
    )(own, sel, q_all, *kv, late)


def combine_kernel(part_ref, out_ref):
    lse = []
    for o in range(OUTER):
        terms = part_ref[o, HD:, :].astype(jnp.float32)
        lse.append(terms[0:1] + terms[1:2] + terms[2:3])
    top = lse[0]
    for o in range(1, OUTER):
        top = jnp.maximum(top, lse[o])
    total = jnp.zeros_like(top)
    acc = jnp.zeros((HD, 2 * QC), jnp.float32)
    for o in range(OUTER):
        w = jnp.exp2(lse[o] - top)
        total = total + w
        acc = acc + w * part_ref[o, :HD, :].astype(jnp.float32)
    mixed = (acc * (1.0 / total)).T
    halves = []
    for at in (0, QC):
        heads = [mixed[at + h * CH : at + (h + 1) * CH] for h in range(GROUP)]
        halves.append(jnp.concatenate(heads, axis=1))
    out_ref[...] = jnp.concatenate(halves, axis=0).astype(jnp.bfloat16)


def combine(parts):
    return pl.pallas_call(
        combine_kernel,
        out_shape=jax.ShapeDtypeStruct((ROWS, GROUP * HD), jnp.bfloat16),
        in_specs=[pl.BlockSpec(memory_space=pltpu.VMEM)],
        out_specs=pl.BlockSpec(memory_space=pltpu.VMEM),
        cost_estimate=pl.CostEstimate(flops=10**8, bytes_accessed=12 * 10**5, transcendentals=0),
        name="combine",
    )(parts)


def project_kernel(place_ref, x_ref, y_ref, w_ref, v_ref, *outs):
    step = pl.program_id(0)
    got = dot(x_ref[...], w_ref[...], ((1,), (0,))) + dot(y_ref[...], v_ref[...], ((1,), (0,)))
    got = got.astype(jnp.bfloat16)
    cuts = outs[0].shape[1] // got.shape[1]
    for n in range(cuts * len(outs)):
        at = (n % cuts) * got.shape[1]

        @pl.when(step == n)
        def _():
            outs[n // cuts][:, at : at + got.shape[1]] = got


def project(blocks, x, y, w_own, w_other, width):
    cuts = OUT // width
    rows, depth = x.shape
    count = blocks.shape[0]

    def block(i, place_ref):
        return (0, place_ref[i // cuts] * cuts + lax.rem(i, cuts))

    return pl.pallas_call(
        project_kernel,
        out_shape=[jax.ShapeDtypeStruct((rows, OUT), jnp.bfloat16)] * count,
        grid_spec=pltpu.PrefetchScalarGridSpec(
            num_scalar_prefetch=1,
            grid=(count * cuts,),
            in_specs=[
                pl.BlockSpec((rows, depth), lambda i, p: (0, 0)),
                pl.BlockSpec((rows, depth), lambda i, p: (0, 0)),
                pl.BlockSpec((depth, width), block),
                pl.BlockSpec((depth, width), block),
            ],
            out_specs=[pl.BlockSpec((rows, OUT), lambda i, p: (0, 0))] * count,
        ),
        compiler_params=pltpu.CompilerParams(dimension_semantics=("arbitrary",)),
        cost_estimate=pl.CostEstimate(
            flops=10 * 2 * rows * 2 * depth * OUT * count,
            bytes_accessed=2 * depth * OUT * count * 2,
            transcendentals=0,
        ),
        name="project",
    )(blocks, x, y, w_own, w_other)


def added(*terms):
    return sum(t.astype(jnp.float32) for t in terms).astype(jnp.bfloat16)


def xor_to(axis, size, mask, x):
    return lax.ppermute(x, axis, [(n, n ^ mask) for n in range(size)])


def shards(queries, keys, values, stretch_order, w_out):
    o = lax.axis_index("outer")
    i = lax.axis_index("inner")
    t = lax.axis_index("tensor")
    z, core = t // 2, t % 2
    ahead = 1 - 2 * core
    hops = jnp.stack([2 + 0 * z, ZHI - ahead, ZHI + ahead, 0 * z]).astype(jnp.int32)
    place = lax.rem(z + hops, ZHI) * 2 + core

    early = stretch_order.reshape(OUTER, INNER, 2)[:, :, 0]
    j = lax.dynamic_index_in_dim(early, i, 1, keepdims=False)
    k_row = lax.dynamic_index_in_dim(early, o, 0, keepdims=False)
    slots = jnp.arange(INNER, dtype=jnp.int32)
    hit = (slots[:, None] ^ i) == slots[None, :]
    k_here = jnp.sum(jnp.where(hit, k_row[None, :], 0), axis=1)
    late = (k_here[None, :] > j[:, None]).astype(jnp.int32)
    late_rows = jnp.broadcast_to(
        jnp.repeat(late, CH, axis=1).astype(jnp.bfloat16)[:, None, :], (OUTER, 16, INNER * CH)
    )

    kv_own = jnp.concatenate([keys, values], axis=0)
    kv_far = xor_to("inner", INNER, FAR, kv_own)
    q_many = jnp.broadcast_to(queries[None], (OUTER,) + queries.shape)
    q_all = lax.all_to_all(q_many, "outer", 0, 0, tiled=True)
    kv_own = jnp.concatenate([kv_own, kv_far], axis=0)
    kv_own, late, late_rows, place = lax.optimization_barrier((kv_own, late, late_rows, place))
    kv = [kv_own] + [xor_to("inner", INNER, s, kv_own) for s in range(1, FAR)]

    q_all, kv, w_send = lax.optimization_barrier((q_all, kv, w_out))
    w_other = xor_to("tensor", 2 * ZHI, 1, w_send)

    part = partial_attention(o.reshape(1), late.reshape(-1), q_all, kv, late_rows, 0)
    part = lax.all_to_all(part, "outer", 0, 0, tiled=True)
    x = combine(part)
    y = xor_to("tensor", 2 * ZHI, 1, x)

    count = 2 * ZHI
    ahead_of = [(n + 2 - 4 * (n % 2)) % count for n in range(count)]
    along = [(n, ahead_of[n]) for n in range(count)]
    against = [(ahead_of[n], n) for n in range(count)]
    (far,) = project(place[:1], x, y, w_out, w_other, 512)
    relay = lax.ppermute(far, "tensor", along)
    behind, front, mine = project(place[1:], x, y, w_out, w_other, 512)
    plain = lax.ppermute(behind, "tensor", against)
    merged = lax.ppermute(added(front, relay), "tensor", along)
    return added(mine, plain, merged)


def solution(mesh):
    placed = (
        P(("outer", "inner"), "tensor"),
        P(("outer", "inner"), "tensor"),
        P(("outer", "inner"), "tensor"),
        P(),
        P("tensor", None),
    )
    return jax.shard_map(
        shards,
        mesh=mesh,
        in_specs=placed,
        out_specs=P(("outer", "inner"), "tensor"),
        check_vma=False,
    )
```

```python
import math

import jax
import jax.numpy as jnp
from jax import lax
from jax.experimental import pallas as pl
from jax.experimental.pallas import tpu as pltpu
from jax.sharding import PartitionSpec as P


HD = 128
HEADS = 4
CH = 64
ROWS = 2 * CH
OUTER = 16
INNER = 8
FAR = 4
ZHI = 4
QC = HEADS * CH
EXTRA = 16
NEG = -1e30
COEF = math.log2(math.e) / math.sqrt(HD)
PER = 4
OUT = 1024


def dot(a, b, dims):
    return lax.dot_general(a, b, (dims, ((), ())), preferred_element_type=jnp.float32)


def three_terms(x):
    hi = x.astype(jnp.bfloat16)
    rest = x - hi.astype(jnp.float32)
    mid = rest.astype(jnp.bfloat16)
    low = (rest - mid.astype(jnp.float32)).astype(jnp.bfloat16)
    return hi.astype(jnp.float32), mid.astype(jnp.float32), low.astype(jnp.float32)


def attention_kernel(own_ref, sel_ref, q_ref, *refs):
    pairs = refs[:FAR]
    late_ref, oe_ref, ol_ref, pick, dense, vt_dense, vt_e, vt_l = refs[FAR:]

    def rows_of(s, at):
        first = (s // FAR) * 2 * ROWS + at
        return pairs[s % FAR][first : first + CH, :]

    step = pl.program_id(0)
    keys_dense = INNER * CH

    @pl.when(step == 0)
    def _():
        zero = jnp.zeros((CH, HD), jnp.bfloat16)
        for s in range(INNER):
            k_e = rows_of(s, 0)
            k_l = rows_of(s, CH)
            pick[s, 0] = jnp.concatenate([k_e, zero], axis=1)
            pick[s, 1] = jnp.concatenate([zero, k_l], axis=1)
            dense[s * CH : (s + 1) * CH, :] = jnp.concatenate([zero, k_e], axis=1)
        dense[keys_dense:, :] = jnp.concatenate([zero, rows_of(0, CH)], axis=1)
        v_e = jnp.concatenate([rows_of(s, ROWS) for s in range(INNER)], axis=0)
        v_l = jnp.concatenate([rows_of(s, ROWS + CH) for s in range(INNER)], axis=0)
        t_e = v_e.astype(jnp.float32).T.astype(jnp.bfloat16)
        t_l = v_l.astype(jnp.float32).T.astype(jnp.bfloat16)
        vt_e[...] = t_e
        vt_l[...] = t_l
        vt_dense[:, :keys_dense] = t_e
        vt_dense[:, keys_dense:] = t_l[:, :CH]

    key_at = lax.broadcasted_iota(jnp.int32, (CH, QC), 0)
    query_at = lax.broadcasted_iota(jnp.int32, (CH, QC), 1) % CH
    causal = key_at <= query_at

    for p in range(PER):
        a = step * PER + p
        own = a == own_ref[0]
        q = q_ref[p]
        stacked = [
            jnp.concatenate([q[r : r + CH, h * HD : (h + 1) * HD] for h in range(HEADS)], axis=0)
            for r in (0, CH)
        ]
        q_cat = jnp.concatenate(stacked, axis=1)
        s_dense = dot(dense[...], q_cat, ((1,), (1,)))
        late = [sel_ref[a * INNER + s] > 0 for s in range(INNER)]
        chosen = jnp.concatenate([pick[s, sel_ref[a * INNER + s]] for s in range(INNER)], axis=0)
        s_sel = dot(chosen, q_cat, ((1,), (1,)))
        keep = jnp.where(own, 1, 0)
        s_first = jnp.where(jnp.logical_or(causal, keep == 0), s_sel[:CH], NEG)
        s_extra = jnp.where(jnp.logical_and(causal, keep == 1), s_dense[keys_dense:], NEG)
        blocks = [s_first] + [s_sel[s * CH : (s + 1) * CH] for s in range(1, INNER)]
        tops = [jnp.max(b, axis=0, keepdims=True) for b in blocks]
        m_e = jnp.full((1, QC), NEG, jnp.float32)
        m_l = jnp.maximum(
            jnp.max(s_dense[:keys_dense], axis=0, keepdims=True),
            jnp.max(s_extra, axis=0, keepdims=True),
        )
        for s in range(INNER):
            m_e = jnp.maximum(m_e, jnp.where(late[s], NEG, tops[s]))
            m_l = jnp.maximum(m_l, jnp.where(late[s], tops[s], NEG))
        p_dense = jnp.exp2((s_dense[:keys_dense] - m_l) * COEF)
        p_extra = jnp.exp2((s_extra - m_l) * COEF)
        l_l = jnp.sum(p_dense, axis=0, keepdims=True) + jnp.sum(p_extra, axis=0, keepdims=True)
        l_e = jnp.zeros((1, QC), jnp.float32)
        weights = []
        for s in range(INNER):
            w = jnp.exp2((blocks[s] - jnp.where(late[s], m_l, m_e)) * COEF)
            part = jnp.sum(w, axis=0, keepdims=True)
            l_e = l_e + jnp.where(late[s], 0.0, part)
            l_l = l_l + jnp.where(late[s], part, 0.0)
            weights.append(w.astype(jnp.bfloat16))
        w_sel = jnp.concatenate(weights, axis=0)
        w_dense = jnp.concatenate([p_dense.astype(jnp.bfloat16), p_extra.astype(jnp.bfloat16)], axis=0)
        is_late = late_ref[p, 0:1, :]
        v_sel = jnp.concatenate([vt_e[...] * (1 - is_late), vt_l[...] * is_late], axis=0)
        o_sel = dot(v_sel, w_sel, ((1,), (0,)))
        o_e = o_sel[:HD]
        o_l = o_sel[HD:] + dot(vt_dense[...], w_dense, ((1,), (0,)))
        some = l_e > 0.0
        inv_e = jnp.where(some, 1.0 / jnp.where(some, l_e, 1.0), 0.0)
        lse_e = jnp.where(some, m_e * COEF + jnp.log2(jnp.where(some, l_e, 1.0)), NEG)
        lse_l = m_l * COEF + jnp.log2(l_l)
        for ref, o_t, inv, lse in ((oe_ref, o_e, inv_e, lse_e), (ol_ref, o_l, 1.0 / l_l, lse_l)):
            rows = list(three_terms(lse)) + [jnp.zeros((EXTRA - 3, QC), jnp.float32)]
            ref[p, :HD, :] = (o_t * inv).astype(jnp.bfloat16)
            ref[p, HD:, :] = jnp.concatenate(rows, axis=0).astype(jnp.bfloat16)


def partial_attention(own, sel, q_all, kv, late):
    n_keys = INNER * CH
    return pl.pallas_call(
        attention_kernel,
        out_shape=[jax.ShapeDtypeStruct((OUTER, HD + EXTRA, QC), jnp.bfloat16)] * 2,
        grid=(OUTER // PER,),
        in_specs=[
            pl.BlockSpec(memory_space=pltpu.SMEM),
            pl.BlockSpec(memory_space=pltpu.SMEM),
            pl.BlockSpec((PER, ROWS, HEADS * HD), lambda i: (i, 0, 0)),
            *[pl.BlockSpec((4 * ROWS, HD), lambda i: (0, 0)) for _ in range(FAR)],
            pl.BlockSpec((PER, 16, n_keys), lambda i: (i, 0, 0)),
        ],
        out_specs=[pl.BlockSpec((PER, HD + EXTRA, QC), lambda i: (i, 0, 0))] * 2,
        scratch_shapes=[
            pltpu.VMEM((INNER, 2, CH, 2 * HD), jnp.bfloat16),
            pltpu.VMEM((n_keys + CH, 2 * HD), jnp.bfloat16),
            pltpu.VMEM((HD, n_keys + CH), jnp.bfloat16),
            pltpu.VMEM((HD, n_keys), jnp.bfloat16),
            pltpu.VMEM((HD, n_keys), jnp.bfloat16),
        ],
        compiler_params=pltpu.CompilerParams(dimension_semantics=("arbitrary",)),
        cost_estimate=pl.CostEstimate(flops=8 * 10**9, bytes_accessed=6 * 10**6, transcendentals=4 * 10**6),
        name="partial_attention",
    )(own, sel, q_all, *kv, late)


def combine_kernel(part_ref, out_ref):
    lse = []
    for o in range(OUTER):
        terms = part_ref[o, HD:, :].astype(jnp.float32)
        lse.append(terms[0:1] + terms[1:2] + terms[2:3])
    top = lse[0]
    for o in range(1, OUTER):
        top = jnp.maximum(top, lse[o])
    total = jnp.zeros_like(top)
    acc = jnp.zeros((HD, QC), jnp.float32)
    for o in range(OUTER):
        w = jnp.exp2(lse[o] - top)
        total = total + w
        acc = acc + w * part_ref[o, :HD, :].astype(jnp.float32)
    mixed = (acc * (1.0 / total)).T
    heads = [mixed[h * CH : (h + 1) * CH] for h in range(HEADS)]
    out_ref[...] = jnp.concatenate(heads, axis=1).astype(jnp.bfloat16)


def combine(parts):
    return pl.pallas_call(
        combine_kernel,
        out_shape=jax.ShapeDtypeStruct((CH, HEADS * HD), jnp.bfloat16),
        in_specs=[pl.BlockSpec(memory_space=pltpu.VMEM)],
        out_specs=pl.BlockSpec(memory_space=pltpu.VMEM),
        cost_estimate=pl.CostEstimate(flops=10**8, bytes_accessed=12 * 10**5, transcendentals=0),
        name="combine",
    )(parts)


def project_kernel(place_ref, x_ref, y_ref, w_ref, v_ref, *outs):
    step = pl.program_id(0)
    got = dot(x_ref[...], w_ref[...], ((1,), (0,))) + dot(y_ref[...], v_ref[...], ((1,), (0,)))
    got = got.astype(jnp.bfloat16)
    cuts = outs[0].shape[1] // got.shape[1]
    for n in range(cuts * len(outs)):
        at = (n % cuts) * got.shape[1]

        @pl.when(step == n)
        def _():
            outs[n // cuts][:, at : at + got.shape[1]] = got


def project(blocks, x, y, w_own, w_other, width):
    cuts = OUT // width
    rows, depth = x.shape
    count = blocks.shape[0]

    def block(i, place_ref):
        return (0, place_ref[i // cuts] * cuts + lax.rem(i, cuts))

    return pl.pallas_call(
        project_kernel,
        out_shape=[jax.ShapeDtypeStruct((rows, OUT), jnp.bfloat16)] * count,
        grid_spec=pltpu.PrefetchScalarGridSpec(
            num_scalar_prefetch=1,
            grid=(count * cuts,),
            in_specs=[
                pl.BlockSpec((rows, depth), lambda i, p: (0, 0)),
                pl.BlockSpec((rows, depth), lambda i, p: (0, 0)),
                pl.BlockSpec((depth, width), block),
                pl.BlockSpec((depth, width), block),
            ],
            out_specs=[pl.BlockSpec((rows, OUT), lambda i, p: (0, 0))] * count,
        ),
        compiler_params=pltpu.CompilerParams(dimension_semantics=("arbitrary",)),
        cost_estimate=pl.CostEstimate(
            flops=10 * 2 * rows * 2 * depth * OUT * count,
            bytes_accessed=2 * depth * OUT * count * 2,
            transcendentals=0,
        ),
        name="project",
    )(blocks, x, y, w_own, w_other)


def added(*terms):
    return sum(t.astype(jnp.float32) for t in terms).astype(jnp.bfloat16)


def xor_to(axis, size, mask, x):
    return lax.ppermute(x, axis, [(n, n ^ mask) for n in range(size)])


def shards(queries, keys, values, stretch_order, w_out):
    o = lax.axis_index("outer")
    i = lax.axis_index("inner")
    t = lax.axis_index("tensor")
    z, core = t // 2, t % 2
    ahead = 1 - 2 * core
    hops = jnp.stack([2 + 0 * z, ZHI - ahead, ZHI + ahead, 0 * z]).astype(jnp.int32)
    place = lax.rem(z + hops, ZHI) * 2 + core

    early = stretch_order.reshape(OUTER, INNER, 2)[:, :, 0]
    j = lax.dynamic_index_in_dim(early, i, 1, keepdims=False)
    k_row = lax.dynamic_index_in_dim(early, o, 0, keepdims=False)
    slots = jnp.arange(INNER, dtype=jnp.int32)
    hit = (slots[:, None] ^ i) == slots[None, :]
    k_here = jnp.sum(jnp.where(hit, k_row[None, :], 0), axis=1)
    late = (k_here[None, :] > j[:, None]).astype(jnp.int32)
    late_rows = jnp.broadcast_to(
        jnp.repeat(late, CH, axis=1).astype(jnp.bfloat16)[:, None, :], (OUTER, 16, INNER * CH)
    )

    kv_own = jnp.concatenate([keys, values], axis=0)
    kv_far = xor_to("inner", INNER, FAR, kv_own)
    q_many = jnp.broadcast_to(queries[None], (OUTER,) + queries.shape)
    q_all = lax.all_to_all(q_many, "outer", 0, 0, tiled=True)
    kv_own = jnp.concatenate([kv_own, kv_far], axis=0)
    kv_own, late, late_rows, place = lax.optimization_barrier((kv_own, late, late_rows, place))
    kv = [kv_own] + [xor_to("inner", INNER, s, kv_own) for s in range(1, FAR)]
    kv, w_send = lax.optimization_barrier((kv, w_out))
    w_other = xor_to("tensor", 2 * ZHI, 1, w_send)

    part_e, part_l = partial_attention(o.reshape(1), late.reshape(-1), q_all, kv, late_rows)
    part_e = lax.all_to_all(part_e, "outer", 0, 0, tiled=True)
    part_e, part_l = lax.optimization_barrier((part_e, part_l))
    part_l = lax.all_to_all(part_l, "outer", 0, 0, tiled=True)

    count = 2 * ZHI
    ahead_of = [(n + 2 - 4 * (n % 2)) % count for n in range(count)]
    along = [(n, ahead_of[n]) for n in range(count)]
    against = [(ahead_of[n], n) for n in range(count)]
    results = []
    for part in (part_e, part_l):
        x = combine(part)
        y = xor_to("tensor", count, 1, x)
        (far,) = project(place[:1], x, y, w_out, w_other, 512)
        relay = lax.ppermute(far, "tensor", along)
        behind, front, mine = project(place[1:], x, y, w_out, w_other, 512)
        plain = lax.ppermute(behind, "tensor", against)
        front = added(front, relay)
        merged = lax.ppermute(front, "tensor", along)
        results.append((mine, plain, merged))
    return jnp.concatenate([added(*r) for r in results], axis=0)


def solution(mesh):
    placed = (
        P(("outer", "inner"), "tensor"),
        P(("outer", "inner"), "tensor"),
        P(("outer", "inner"), "tensor"),
        P(),
        P("tensor", None),
    )
    return jax.shard_map(
        shards,
        mesh=mesh,
        in_specs=placed,
        out_specs=P(("outer", "inner"), "tensor"),
        check_vma=False,
    )
```

```python
import functools
import math

import jax
import jax.numpy as jnp
from jax import lax
from jax.experimental import pallas as pl
from jax.experimental.pallas import tpu as pltpu
from jax.sharding import PartitionSpec as P


HD = 128
HEADS = 4
CH = 64
ROWS = 2 * CH
OUTER = 16
INNER = 8
FAR = 4
ZHI = 4
QC = HEADS * CH
EXTRA = 16
NEG = -1e30
COEF = math.log2(math.e) / math.sqrt(HD)
PER = 8
OUT = 1024


def dot(a, b, dims):
    return lax.dot_general(a, b, (dims, ((), ())), preferred_element_type=jnp.float32)


def three_terms(x):
    hi = x.astype(jnp.bfloat16)
    rest = x - hi.astype(jnp.float32)
    mid = rest.astype(jnp.bfloat16)
    low = (rest - mid.astype(jnp.float32)).astype(jnp.bfloat16)
    return hi.astype(jnp.float32), mid.astype(jnp.float32), low.astype(jnp.float32)


def attention_kernel(late, own_ref, on_ref, q_ref, *refs):
    pairs = refs[:FAR]
    out_ref, k_all, v_all = refs[FAR:]
    step = pl.program_id(0)
    span = INNER * CH
    free = span if late else 0

    def rows_of(s, at):
        first = (s // FAR) * 2 * ROWS + at
        return pairs[s % FAR][first : first + CH, :]

    @pl.when(step == 0)
    def _():
        for first, at in ((0, 0), (free, CH)) if late else ((0, 0),):
            for s in range(INNER):
                k_all[first + s * CH : first + (s + 1) * CH, :] = rows_of(s, at)
            v = jnp.concatenate([rows_of(s, ROWS + at) for s in range(INNER)], axis=0)
            v_all[:, first : first + span] = v.astype(jnp.float32).T.astype(jnp.bfloat16)

    key_at = lax.broadcasted_iota(jnp.int32, (CH, QC), 0)
    query_at = lax.broadcasted_iota(jnp.int32, (CH, QC), 1) % CH
    causal = key_at <= query_at

    spread = []
    for p in range(PER):
        q = q_ref[p]
        q = jnp.concatenate([q[:, h * HD : (h + 1) * HD] for h in range(HEADS)], axis=0)
        spread.append(dot(k_all[...], q, ((1,), (1,))))
    tops, totals, weights = [], [], []
    for p in range(PER):
        a = step * PER + p
        away = jnp.where(a == own_ref[0], 0, 1)
        scores = spread[p]
        blocks = [scores[:free]] if late else []
        for s in range(INNER):
            block = scores[free + s * CH : free + (s + 1) * CH]
            if s == 0:
                block = jnp.where(jnp.logical_or(causal, away > 0), block, NEG)
            blocks.append(jnp.where(on_ref[a * INNER + s] > 0, block, NEG))
        scores = jnp.concatenate(blocks, axis=0)
        tops.append(jnp.max(scores, axis=0, keepdims=True))
        w = jnp.exp2((scores - tops[p]) * COEF)
        totals.append(jnp.sum(w, axis=0, keepdims=True))
        weights.append(w.astype(jnp.bfloat16))
    sums = [dot(v_all[...], weights[p], ((1,), (0,))) for p in range(PER)]
    for p in range(PER):
        lse = tops[p] * COEF + jnp.log2(totals[p])
        rows = list(three_terms(lse)) + [jnp.zeros((EXTRA - 3, QC), jnp.float32)]
        out_ref[p, :HD, :] = (sums[p] * (1.0 / totals[p])).astype(jnp.bfloat16)
        out_ref[p, HD:, :] = jnp.concatenate(rows, axis=0).astype(jnp.bfloat16)


def partial_attention(late, own, on, q_all, kv):
    n_keys = INNER * CH * (2 if late else 1)
    return pl.pallas_call(
        functools.partial(attention_kernel, late),
        out_shape=jax.ShapeDtypeStruct((OUTER, HD + EXTRA, QC), jnp.bfloat16),
        grid=(OUTER // PER,),
        in_specs=[
            pl.BlockSpec(memory_space=pltpu.SMEM),
            pl.BlockSpec(memory_space=pltpu.SMEM),
            pl.BlockSpec((PER, CH, HEADS * HD), lambda i: (i, 1 if late else 0, 0)),
            *[pl.BlockSpec((4 * ROWS, HD), lambda i: (0, 0)) for _ in range(FAR)],
        ],
        out_specs=pl.BlockSpec((PER, HD + EXTRA, QC), lambda i: (i, 0, 0)),
        scratch_shapes=[
            pltpu.VMEM((n_keys, HD), jnp.bfloat16),
            pltpu.VMEM((HD, n_keys), jnp.bfloat16),
        ],
        compiler_params=pltpu.CompilerParams(dimension_semantics=("arbitrary",)),
        cost_estimate=pl.CostEstimate(flops=8 * 10**9, bytes_accessed=3 * 10**6, transcendentals=4 * 10**6),
        name="attend_late" if late else "attend_early",
    )(own, on, q_all, *kv)


def combine_kernel(part_ref, out_ref):
    lse = []
    for o in range(OUTER):
        terms = part_ref[o, HD:, :].astype(jnp.float32)
        lse.append(terms[0:1] + terms[1:2] + terms[2:3])
    top = lse[0]
    for o in range(1, OUTER):
        top = jnp.maximum(top, lse[o])
    total = jnp.zeros_like(top)
    acc = jnp.zeros((HD, QC), jnp.float32)
    for o in range(OUTER):
        w = jnp.exp2(lse[o] - top)
        total = total + w
        acc = acc + w * part_ref[o, :HD, :].astype(jnp.float32)
    mixed = (acc * (1.0 / total)).T
    heads = [mixed[h * CH : (h + 1) * CH] for h in range(HEADS)]
    out_ref[...] = jnp.concatenate(heads, axis=1).astype(jnp.bfloat16)


def combine(parts):
    return pl.pallas_call(
        combine_kernel,
        out_shape=jax.ShapeDtypeStruct((CH, HEADS * HD), jnp.bfloat16),
        in_specs=[pl.BlockSpec(memory_space=pltpu.VMEM)],
        out_specs=pl.BlockSpec(memory_space=pltpu.VMEM),
        cost_estimate=pl.CostEstimate(flops=10**8, bytes_accessed=12 * 10**5, transcendentals=0),
        name="combine",
    )(parts)


def project_kernel(place_ref, x_ref, y_ref, w_ref, v_ref, *outs):
    step = pl.program_id(0)
    got = dot(x_ref[...], w_ref[...], ((1,), (0,))) + dot(y_ref[...], v_ref[...], ((1,), (0,)))
    got = got.astype(jnp.bfloat16)
    cuts = outs[0].shape[1] // got.shape[1]
    for n in range(cuts * len(outs)):
        at = (n % cuts) * got.shape[1]

        @pl.when(step == n)
        def _():
            outs[n // cuts][:, at : at + got.shape[1]] = got


def project(blocks, x, y, w_own, w_other, width):
    cuts = OUT // width
    rows, depth = x.shape
    count = blocks.shape[0]

    def block(i, place_ref):
        return (0, place_ref[i // cuts] * cuts + lax.rem(i, cuts))

    return pl.pallas_call(
        project_kernel,
        out_shape=[jax.ShapeDtypeStruct((rows, OUT), jnp.bfloat16)] * count,
        grid_spec=pltpu.PrefetchScalarGridSpec(
            num_scalar_prefetch=1,
            grid=(count * cuts,),
            in_specs=[
                pl.BlockSpec((rows, depth), lambda i, p: (0, 0)),
                pl.BlockSpec((rows, depth), lambda i, p: (0, 0)),
                pl.BlockSpec((depth, width), block),
                pl.BlockSpec((depth, width), block),
            ],
            out_specs=[pl.BlockSpec((rows, OUT), lambda i, p: (0, 0))] * count,
        ),
        compiler_params=pltpu.CompilerParams(dimension_semantics=("arbitrary",)),
        cost_estimate=pl.CostEstimate(
            flops=10 * 2 * rows * 2 * depth * OUT * count,
            bytes_accessed=2 * depth * OUT * count * 2,
            transcendentals=0,
        ),
        name="project",
    )(blocks, x, y, w_own, w_other)


def burst_kernel(place_ref, x_ref, y_ref, w_ref, v_ref, *refs):
    count = len(refs) - 3
    outs, (w_buf, v_buf, sems) = refs[:count], refs[count:]
    width = w_buf.shape[2]
    cuts = OUT // width
    copies = []
    for n in range(count * cuts):
        at = place_ref[n // cuts] * OUT + (n % cuts) * width
        span = pl.ds(pl.multiple_of(at, 128), width)
        copies.append((
            pltpu.make_async_copy(w_ref.at[:, span], w_buf.at[n], sems.at[n, 0]),
            pltpu.make_async_copy(v_ref.at[:, span], v_buf.at[n], sems.at[n, 1]),
        ))
    for pair in copies:
        pair[0].start()
        pair[1].start()
    for n in range(count * cuts):
        copies[n][0].wait()
        copies[n][1].wait()
        got = dot(x_ref[...], w_buf[n], ((1,), (0,))) + dot(y_ref[...], v_buf[n], ((1,), (0,)))
        at = (n % cuts) * width
        outs[n // cuts][:, at : at + width] = got.astype(jnp.bfloat16)


def project_burst(blocks, x, y, w_own, w_other, width):
    rows, depth = x.shape
    count = blocks.shape[0]
    parts = count * (OUT // width)
    vmem = pl.BlockSpec(memory_space=pltpu.VMEM)
    hbm = pl.BlockSpec(memory_space=pl.ANY)
    return pl.pallas_call(
        burst_kernel,
        out_shape=[jax.ShapeDtypeStruct((rows, OUT), jnp.bfloat16)] * count,
        in_specs=[pl.BlockSpec(memory_space=pltpu.SMEM), vmem, vmem, hbm, hbm],
        out_specs=[vmem] * count,
        scratch_shapes=[
            pltpu.VMEM((parts, depth, width), jnp.bfloat16),
            pltpu.VMEM((parts, depth, width), jnp.bfloat16),
            pltpu.SemaphoreType.DMA((parts, 2)),
        ],
        cost_estimate=pl.CostEstimate(
            flops=10 * 2 * rows * 2 * depth * OUT * count,
            bytes_accessed=2 * depth * OUT * count * 2,
            transcendentals=0,
        ),
        name="project_burst",
    )(blocks, x, y, w_own, w_other)


def added(*terms):
    return sum(t.astype(jnp.float32) for t in terms).astype(jnp.bfloat16)


def xor_to(axis, size, mask, x):
    return lax.ppermute(x, axis, [(n, n ^ mask) for n in range(size)])


def shards(queries, keys, values, stretch_order, w_out):
    o = lax.axis_index("outer")
    i = lax.axis_index("inner")
    t = lax.axis_index("tensor")
    z, core = t // 2, t % 2
    ahead = 1 - 2 * core
    hops = jnp.stack([2 + 0 * z, ZHI - ahead, ZHI + ahead, 0 * z]).astype(jnp.int32)
    place = lax.rem(z + hops, ZHI) * 2 + core

    early = stretch_order.reshape(OUTER, INNER, 2)[:, :, 0]
    j = lax.dynamic_index_in_dim(early, i, 1, keepdims=False)
    k_row = lax.dynamic_index_in_dim(early, o, 0, keepdims=False)
    slots = jnp.arange(INNER, dtype=jnp.int32)
    hit = (slots[:, None] ^ i) == slots[None, :]
    k_here = jnp.sum(jnp.where(hit, k_row[None, :], 0), axis=1)
    ons = [(k_here[None, :] <= j[:, None]), (k_here[None, :] >= j[:, None])]
    ons = [on.astype(jnp.int32).reshape(-1) for on in ons]

    kv_own = jnp.concatenate([keys, values], axis=0)
    q_many = jnp.broadcast_to(queries[None], (OUTER,) + queries.shape)
    kv_own, q_many = lax.optimization_barrier((kv_own, q_many))
    kv_far = xor_to("inner", INNER, FAR, kv_own)
    q_all = lax.all_to_all(q_many, "outer", 0, 0, tiled=True)
    kv_own = jnp.concatenate([kv_own, kv_far], axis=0)
    kv_own, ons, place = lax.optimization_barrier((kv_own, ons, place))
    kv = [kv_own] + [xor_to("inner", INNER, s, kv_own) for s in range(1, FAR)]
    own = o.reshape(1)
    part_e = partial_attention(False, own, ons[0], q_all, kv)
    part_e, w_send = lax.optimization_barrier((part_e, w_out))
    w_other = xor_to("tensor", 2 * ZHI, 1, w_send)
    part_e = lax.all_to_all(part_e, "outer", 0, 0, tiled=True)
    part_l = partial_attention(True, own, ons[1], q_all, kv)
    part_e, part_l = lax.optimization_barrier((part_e, part_l))
    part_l = lax.all_to_all(part_l, "outer", 0, 0, tiled=True)

    count = 2 * ZHI
    ahead_of = [(n + 2 - 4 * (n % 2)) % count for n in range(count)]
    along = [(n, ahead_of[n]) for n in range(count)]
    against = [(ahead_of[n], n) for n in range(count)]
    results = []
    for part in (part_e, part_l):
        x = combine(part)
        y = xor_to("tensor", count, 1, x)
        (far,) = project(place[:1], x, y, w_out, w_other, 512)
        relay = lax.ppermute(far, "tensor", along)
        behind, front, mine = project_burst(place[1:], x, y, w_out, w_other, 512)
        plain = lax.ppermute(behind, "tensor", against)
        front = added(front, relay)
        merged = lax.ppermute(front, "tensor", along)
        results.append((mine, plain, merged))
    return jnp.concatenate([added(*r) for r in results], axis=0)


def solution(mesh):
    placed = (
        P(("outer", "inner"), "tensor"),
        P(("outer", "inner"), "tensor"),
        P(("outer", "inner"), "tensor"),
        P(),
        P("tensor", None),
    )
    return jax.shard_map(
        shards,
        mesh=mesh,
        in_specs=placed,
        out_specs=P(("outer", "inner"), "tensor"),
        check_vma=False,
    )
```
